256 devices in a mesh: shard: 64 (over z, y, core), tp: 4 (over x).
Axes of the slice: x: 4, y: 4, z: 8, core: 2. Of those that a mesh axis runs over, the one named last changes fastest.
Arguments:
- weight_query: bfloat16 [12288, 12288], P('shard', 'tp'), may hold values from -0.15625 to 0.15625
- low_query: bfloat16 [12288, 64], P('shard'), may hold values from -0.0546875 to 0.0546875
- high_query: bfloat16 [64, 12288], P(None, 'tp'), may hold values from -0.75 to 0.75
- weight_key: bfloat16 [12288, 12288], P('shard', 'tp'), may hold values from -0.15625 to 0.15625
- low_key: bfloat16 [12288, 64], P('shard'), may hold values from -0.0546875 to 0.0546875
- high_key: bfloat16 [64, 12288], P(None, 'tp'), may hold values from -0.75 to 0.75
- weight_value: bfloat16 [12288, 12288], P('shard', 'tp'), may hold values from -0.15625 to 0.15625
- low_value: bfloat16 [12288, 64], P('shard'), may hold values from -0.0546875 to 0.0546875
- high_value: bfloat16 [64, 12288], P(None, 'tp'), may hold values from -0.75 to 0.75
- norm_train: float32 [12288], P(('shard', 'tp')), may hold values from 0.25 to 1.75
- norm_step: float32 [12288], P(('shard', 'tp')), may hold values from -0.3 to 0.3
Outputs:
- ready_query: bfloat16 [12288, 12288], P(None, ('tp', 'shard'))
- ready_key: bfloat16 [12288, 12288], P(None, ('tp', 'shard'))
- ready_value: bfloat16 [12288, 12288], P(None, ('tp', 'shard'))
- column_query: float32 [12288], P(('tp', 'shard'))
- column_key: float32 [12288], P(('tp', 'shard'))
- column_value: float32 [12288], P(('tp', 'shard'))
- serve_norm: bfloat16 [12288], replicated
The draws below stay inside these ranges and needn't reach their ends.
All inputs are finite; a program needn't handle non-finite values. Where the reference program divides by a largest or mean magnitude, that divisor is 1e-20 or more.
Results may differ from the reference program's by a relative error of at most 0.001.
Values may be sent and summed in bfloat16 or wider, within the bound.
A program may use at most 64 MiB of HBM per device.

```python
import jax
import jax.numpy as jnp

D_MODEL = 12288
Q_DIM = 12288
KV_DIM = 12288
RANK = 64


def with_spikes(values, key, source, target, parts, factor):
    owner, partner = [(jnp.arange(values.shape[position]) // (values.shape[position] // parts)).reshape([-1 if axis == position else 1 for axis in range(values.ndim)]) for position in (source, target)]
    chosen = jax.random.permutation(key, parts)[partner]
    strong = (owner == chosen) | (owner == (partner + parts // 2) % parts)
    return jnp.where(strong, factor * values, values)


def levels(stream_key, dims, shards, smallest, largest):
    loudness = 1.0
    for dim, parts in shards:
        draws = jax.random.uniform(jax.random.fold_in(jax.random.fold_in(stream_key, 6), dim), (parts,), jnp.float32, smallest / len(shards), largest / len(shards))
        loudness = loudness * jnp.repeat(jnp.exp(draws), dims[dim] // parts).reshape((-1,) + (1,) * (len(dims) - 1 - dim))
    return loudness


def bell_draw(key, extent, spread, bound, cuts=(), kind=jnp.bfloat16):
    loudness = levels(key, extent, cuts, -0.22, 0.18) if cuts else 1.0
    values = jax.random.normal(key, extent, jnp.float32) * spread * loudness
    return jnp.minimum(jnp.maximum(values, -bound), bound).astype(kind)


def heavy_noise(key, extent, width, most, shards, heavy, kind=jnp.bfloat16):
    array = width * jax.random.normal(key, extent, jnp.float32)
    if shards:
        array = array * levels(key, extent, shards, -0.22, 0.18)
    return jnp.clip(with_spikes(array, jax.random.fold_in(key, 3), *heavy), -most, most).astype(kind)


def setup_inputs(seed: int = 0) -> dict:
    seeds = jax.random.split(jax.random.key(seed), 12)
    return {
        "weight_query": heavy_noise(seeds[0], (D_MODEL, Q_DIM), D_MODEL ** -0.5, 0.15625, ((0, 64), (1, 4)), (0, 1, 64, 4.0)),
        "low_query": bell_draw(seeds[1], (D_MODEL, RANK), D_MODEL ** -0.5, 0.0546875, ((0, 64),)),
        "high_query": bell_draw(seeds[2], (RANK, Q_DIM), RANK ** -0.5, 0.75, ((1, 4),)),
        "weight_key": heavy_noise(seeds[3], (D_MODEL, KV_DIM), D_MODEL ** -0.5, 0.15625, ((0, 64), (1, 4)), (0, 1, 64, 4.0)),
        "low_key": bell_draw(seeds[4], (D_MODEL, RANK), D_MODEL ** -0.5, 0.0546875, ((0, 64),)),
        "high_key": bell_draw(seeds[5], (RANK, KV_DIM), RANK ** -0.5, 0.75, ((1, 4),)),
        "weight_value": heavy_noise(seeds[6], (D_MODEL, KV_DIM), D_MODEL ** -0.5, 0.15625, ((0, 64), (1, 4)), (0, 1, 64, 4.0)),
        "low_value": bell_draw(seeds[7], (D_MODEL, RANK), D_MODEL ** -0.5, 0.0546875, ((0, 64),)),
        "high_value": bell_draw(seeds[8], (RANK, KV_DIM), RANK ** -0.5, 0.75, ((1, 4),)),
        "norm_train": jnp.clip(1.0 + 0.15 * jax.random.normal(seeds[9], (D_MODEL,), jnp.float32), 0.25, 1.75),
        "norm_step": jnp.clip(jax.random.uniform(seeds[10], (D_MODEL,), jnp.float32, -0.3, 0.3) * levels(seeds[10], (D_MODEL,), ((0, 256),), -0.4, 0.0), -0.3, 0.3),
    }


mix_rate = 0.5


def reference(weight_query, low_query, high_query, weight_key, low_key, high_key, weight_value, low_value, high_value, norm_train, norm_step):
    latest_query = weight_query.astype(jnp.float32) + mix_rate * jnp.dot(low_query, high_query, preferred_element_type=jnp.float32)
    latest_key = weight_key.astype(jnp.float32) + mix_rate * jnp.dot(low_key, high_key, preferred_element_type=jnp.float32)
    latest_value = weight_value.astype(jnp.float32) + mix_rate * jnp.dot(low_value, high_value, preferred_element_type=jnp.float32)
    column_query = jnp.sum(jnp.abs(latest_query), axis=0) / D_MODEL
    ready_query = (latest_query / column_query).astype(jnp.bfloat16)
    column_key = jnp.sum(jnp.abs(latest_key), axis=0) / D_MODEL
    ready_key = (latest_key / column_key).astype(jnp.bfloat16)
    column_value = jnp.sum(jnp.abs(latest_value), axis=0) / D_MODEL
    ready_value = (latest_value / column_value).astype(jnp.bfloat16)
    serve_norm = (norm_train + norm_step).astype(jnp.bfloat16)
    return ready_query, ready_key, ready_value, column_query, column_key, column_value, serve_norm
```

```python
import jax
import jax.numpy as jnp
from jax import lax
from jax.experimental import pallas as pl
from jax.experimental.pallas import tpu as pltpu
from jax.sharding import Mesh
from jax.sharding import PartitionSpec as P

D_MODEL = 12288
MIX_RATE = 0.5
MESH = pl.DeviceIdType.MESH
SIZES = {"z": 8, "y": 4, "c": 2, "x": 4}
ROWS = 192
TILE = 128
TILES = 9
UNITS = 36
Z_ORDER = (4, 3, 5, 2, 6, 1, 7)
PIECES = (
    ((0, 0, 0, 48), (1, 48, 0, 48), (2, 96, 0, 32)),
    ((2, 0, 32, 16), (3, 16, 0, 48), (4, 64, 0, 48), (5, 112, 0, 16)),
    ((5, 0, 16, 32), (6, 32, 0, 48), (7, 80, 0, 48)),
)
EARLY = 1


def shifted(**offsets):
    return {a: lax.rem(lax.axis_index(a) + o, SIZES[a]) for a, o in offsets.items()}


def all_peers():
    out = [{"z": dz, "c": dc} for dz in range(8) for dc in range(2) if dz or dc]
    out += [{"x": dx, "c": dc} for dx in range(1, 4) for dc in range(2)]
    out += [{"y": dy, "c": dc} for dy in range(1, 4) for dc in range(2)]
    return out


def remote(src, dst, send, recv, device):
    return pltpu.make_async_remote_copy(
        src_ref=src, dst_ref=dst, send_sem=send, recv_sem=recv, device_id=device, device_id_type=MESH
    )


def wait_bytes(ref, sem):
    pltpu.make_async_copy(ref, ref, sem).wait()


def product(low, high):
    return lax.dot_general(low, high, (((0,), (0,)), ((), ())), preferred_element_type=jnp.float32)


def kernel(
    wq, lq, hq, wk, lk, hk, wv, lv, hv, nt, ns,
    out, cols, norm,
    weights, highs, lows, units, ready, quarters, part, got1, got2, total, norms, gathered, mean, wide,
    w_sem, h_sem, l_sem, q_sem, own_sem,
    unit_sem, z_send, c_send,
    low_send, low_recv, low_send2, low_recv2,
    s1_send, s1_recv, s2_send, s2_recv, s3_send, s3_recv, n3_send, n3_recv, n4_send, n4_recv,
    y_send, y_recv,
):
    z, y, c, x = (lax.axis_index(a) for a in ("z", "y", "c", "x"))
    member = 2 * y + c
    w_in, l_in, h_in = (wq, wk, wv), (lq, lk, lv), (hq, hk, hv)

    barrier = pltpu.get_barrier_semaphore()
    peers = all_peers()
    for p in peers:
        pl.semaphore_signal(barrier, inc=1, device_id=shifted(**p), device_id_type=MESH)

    loads = []
    for t in range(3):
        loads.append(
            (
                pltpu.make_async_copy(w_in[t], weights.at[t], w_sem.at[t]),
                pltpu.make_async_copy(h_in[t], highs.at[t], h_sem.at[t]),
                pltpu.make_async_copy(l_in[t], lows.at[t], l_sem.at[t]),
            )
        )
        for copy in loads[t]:
            copy.start()
    quarter = quarters.at[4 * c + x, 0]
    quarter_loads = []
    for t in range(3):
        copy = pltpu.make_async_copy(
            l_in[t].at[pl.ds(pl.multiple_of(16 * x, 16), 16), :],
            quarter.at[pl.ds(16 * t, 16), :],
            q_sem.at[t],
        )
        copy.start()
        quarter_loads.append(copy)

    def slot_of(k, tile):
        return 4 * k + tile // 2 if tile < 8 else 32 + k // 2

    def half(slot, core):
        return units.at[pl.ds(pl.multiple_of(384 * slot + ROWS * core, 64), ROWS), :]

    def slab(k, tile):
        first = 384 * lax.rem(z + k, 8) + TILE * (tile % 3)
        return weights.at[tile // 3, :, pl.ds(pl.multiple_of(first, TILE), TILE)]

    def slab_in(tile):
        first = 384 * z + TILE * (tile % 3)
        return w_in[tile // 3].at[:, pl.ds(pl.multiple_of(first, TILE), TILE)]

    for tile in range(TILES):

        @pl.when(c == tile % 2)
        def _():
            slot = slot_of(0, tile)
            pltpu.make_async_copy(slab_in(tile), half(slot, c), unit_sem.at[slot]).start()

    for t in range(3):
        for copy in loads[t]:
            copy.wait()
        low = lows[t]

        def sums(s, _):
            for j in range(3):
                first = pl.ds(pl.multiple_of(384 * s + TILE * j, TILE), TILE)
                latest = weights[t, :, first].astype(jnp.float32) + MIX_RATE * product(low, highs[t, :, first])
                part[s, pl.ds(3 * t + j, 1), :] = jnp.sum(jnp.abs(latest), axis=0, keepdims=True)
            return 0

        lax.fori_loop(0, 8, sums, 0)
    own_norm = jnp.concatenate([nt[...] + ns[...], jnp.zeros((1, 80), jnp.float32)], axis=1)
    for s in range(8):
        part[s, pl.ds(9, 1), :] = own_norm
    for copy in quarter_loads:
        copy.wait()

    pl.semaphore_wait(barrier, len(peers))

    for k in Z_ORDER:
        remote(quarter, quarters.at[4 * c + x, k], low_send, low_recv, shifted(z=k)).start()
    for tile in range(TILES):

        @pl.when(c != tile % 2)
        def _():
            slot = slot_of(0, tile)
            remote(slab(0, tile), half(slot, c), c_send, unit_sem.at[slot], shifted(c=1)).start()

    def send_round(tile):
        for k in Z_ORDER:
            slot = slot_of(k, tile)
            device = {"z": lax.rem(z + k, 8), "c": (k + tile) % 2}
            remote(slab(k, tile), half(slot, c), z_send, unit_sem.at[slot], device).start()

    for tile in range(EARLY):
        send_round(tile)

    for dy in range(4):
        for dc in range(2):
            if dy or dc:
                to = shifted(y=dy, c=dc)
                remote(part.at[2 * to["y"] + to["c"]], got1.at[member], s1_send, s1_recv, to).start()
    got1[member] = part[member]
    wait_bytes(got1.at[pl.ds(0, 7)], s1_recv)
    mine = got1[0]
    for m in range(1, 8):
        mine = mine + got1[m]
    got2[0, pl.ds(0, 16), :] = mine
    for m in range(8):
        got2[0, pl.ds(16 + m, 1), :] = got1[m, pl.ds(9, 1), :]

    steps = lax.rem(member + 8 - z, 8)

    @pl.when(steps != 0)
    def _():
        remote(got2.at[0], got2.at[steps], s2_send, s2_recv, {"z": member}).start()

    for tile in range(EARLY, TILES):
        send_round(tile)

    wait_bytes(quarters.at[0, pl.ds(0, 7)], low_recv)
    for dx in range(4):
        for dc in range(2):
            if dx or dc:
                place = quarters.at[4 * c + x]
                remote(place, place, low_send2, low_recv2, shifted(x=dx, c=dc)).start()

    @pl.when(steps == 0)
    def _():
        wait_bytes(got2.at[pl.ds(0, 7)], s2_recv)
        whole = got2[0, pl.ds(0, 16), :]
        for k in range(1, 8):
            whole = whole + got2[k, pl.ds(0, 16), :]
        total[...] = whole
        for k in range(8):
            plane = lax.rem(z + 8 - k, 8)
            norms[x, pl.ds(pl.multiple_of(8 * plane, 8), 8), :] = got2[k, pl.ds(16, 8), :]
        for src, dst, send, recv in (
            (total, total, s3_send, s3_recv),
            (norms.at[x], norms.at[x], n3_send, n3_recv),
        ):
            n = 0
            for dy in range(4):
                for dc in range(2):
                    if dy or dc:
                        remote(src, dst, send.at[n], recv, shifted(y=dy, c=dc)).start()
                        n += 1

    @pl.when(steps != 0)
    def _():
        wait_bytes(total, s3_recv)
        wait_bytes(norms.at[x], n3_recv)

    for n, dx in enumerate((1, 2, 3)):
        remote(norms.at[x], norms.at[x], n4_send, n4_recv, shifted(x=dx)).start()
    mean[...] = total[...] / D_MODEL
    wait_bytes(quarters.at[pl.ds(0, 7)], low_recv2)

    def unit(n):
        i, j = n // 8, n % 8
        last = n >= 32
        k = jnp.where(last, 2 * (n - 32) + c, jnp.where(j < 4, 2 * j + c, 2 * (j - 4) + 1 - c))
        tile = jnp.where(last, 8, 2 * i + jnp.where(j < 4, 0, 1))
        slot = jnp.where(last, 32 + k // 2, 4 * k + i)
        return k, tile, slot

    def work(n):
        k, tile, slot = unit(n)
        tensor = tile // 3
        here = pl.ds(pl.multiple_of(384 * slot, 128), 384)
        wait_bytes(units.at[here, :], unit_sem.at[slot])
        first = 384 * z + TILE * (tile % 3)
        high = highs[tensor, :, pl.ds(pl.multiple_of(first, TILE), TILE)]
        rank = pl.ds(pl.multiple_of(16 * tensor, 16), 16)
        low = [
            jnp.concatenate([quarters[4 * core + q, k, rank, :] for q in range(4)], axis=0) for core in range(2)
        ]
        added = jnp.concatenate([product(a, high) for a in low], axis=0)
        latest = units[here, :].astype(jnp.float32) + MIX_RATE * added
        scaled = latest / mean[pl.ds(tile, 1), :]
        ready[pl.ds(pl.multiple_of(TILE * slot, TILE), TILE), :] = scaled.astype(jnp.bfloat16).T

    def hand_on(n):
        k, tile, slot = unit(n)
        tensor = tile // 3
        chip = 4 * lax.rem(z + 8 - k, 8) + y
        lanes = pl.ds(pl.multiple_of(384 * chip, 128), 384)
        for t in range(3):

            @pl.when(tile % 3 == t)
            def _():
                for owner, row, column, length in PIECES[t]:
                    src = ready.at[pl.ds(pl.multiple_of(TILE * slot + row, 16), length), :]
                    dst = out.at[tensor, pl.ds(column, length), lanes]

                    @pl.when(member == owner)
                    def _():
                        pltpu.make_async_copy(src, dst, y_recv.at[tensor]).start()

                    @pl.when(member != owner)
                    def _():
                        to = {"y": owner // 2, "c": owner % 2}
                        remote(src, dst, y_send, y_recv.at[tensor], to).start()

    def step(n, _):
        work(n)

        @pl.when(n > 0)
        def _():
            hand_on(n - 1)

        return 0

    lax.fori_loop(0, UNITS, step, 0)
    hand_on(UNITS - 1)

    for m in range(8):

        @pl.when(member == m)
        def _():
            for t in range(3):
                rows = [mean[pl.ds(3 * t + j, 1), :] for j in range(3)]
                line = jnp.concatenate(rows, axis=1)
                cols[pl.ds(t, 1), pl.ds(0, 48)] = line[:, 48 * m : 48 * m + 48]

    wait_bytes(norms.at[pl.ds(0, 3)], n4_recv)
    place = lax.broadcasted_iota(jnp.int32, (64, TILE), 1)
    n0, n1, n2, n3 = (norms[i] for i in range(4))
    r1, r2, r3 = pltpu.roll(n1, 48, 1), pltpu.roll(n2, 96, 1), pltpu.roll(n3, 16, 1)
    gathered[0] = jnp.where(place < 48, n0, jnp.where(place < 96, r1, r2))
    gathered[1] = jnp.where(place < 16, r2, r3)
    even, odd = pl.ds(0, 32, stride=2), pl.ds(1, 32, stride=2)
    a0, a1, b0, b1 = gathered[0, even, :], gathered[0, odd, :], gathered[1, even, :], gathered[1, odd, :]
    low_half = lax.broadcasted_iota(jnp.int32, (32, TILE), 1) < 64
    wide[pl.ds(0, 32, stride=3), :] = a0
    wide[pl.ds(1, 32, stride=3), :] = jnp.where(low_half, b0, pltpu.roll(a1, 64, 1))
    wide[pl.ds(2, 32, stride=3), :] = jnp.where(low_half, pltpu.roll(a1, 64, 1), pltpu.roll(b1, 64, 1))
    norm[...] = wide[...].astype(jnp.bfloat16)

    for t in range(3):
        wait_bytes(out.at[t], y_recv.at[t])
    wait_bytes(ready.at[pl.ds(0, 4032), :], y_send)
    wait_bytes(units.at[pl.ds(0, 63 * ROWS), :], z_send)

    @pl.when(c == 0)
    def _():
        wait_bytes(units.at[pl.ds(0, 4 * ROWS), :], c_send)

    @pl.when(c != 0)
    def _():
        wait_bytes(units.at[pl.ds(0, 5 * ROWS), :], c_send)

    wait_bytes(quarters.at[0, pl.ds(0, 7)], low_send)
    wait_bytes(quarters.at[pl.ds(0, 7)], low_send2)
    wait_bytes(got1.at[pl.ds(0, 7)], s1_send)
    wait_bytes(norms.at[pl.ds(0, 3)], n4_send)

    @pl.when(steps != 0)
    def _():
        wait_bytes(got2.at[0], s2_send)

    @pl.when(steps == 0)
    def _():
        for n in range(7):
            wait_bytes(total, s3_send.at[n])
            wait_bytes(norms.at[0], n3_send.at[n])


def body(wq, lq, hq, wk, lk, hk, wv, lv, hv, nt, ns):
    anywhere = pl.BlockSpec(memory_space=pl.ANY)
    local = pl.BlockSpec(memory_space=pltpu.VMEM)
    dma = pltpu.SemaphoreType.DMA
    bf16, f32 = jnp.bfloat16, jnp.float32
    out, cols, norm = pl.pallas_call(
        kernel,
        name="merge_and_place",
        out_shape=(
            jax.ShapeDtypeStruct((3, 48, D_MODEL), bf16),
            jax.ShapeDtypeStruct((8, TILE), f32),
            jax.ShapeDtypeStruct((96, TILE), bf16),
        ),
        in_specs=[anywhere] * 9 + [local] * 2,
        out_specs=(anywhere, local, local),
        scratch_shapes=[
            pltpu.VMEM((3, ROWS, 3072), bf16),
            pltpu.VMEM((3, 64, 3072), bf16),
            pltpu.VMEM((3, 64, ROWS), bf16),
            pltpu.VMEM((UNITS * 384, TILE), bf16),
            pltpu.VMEM((UNITS * TILE, 384), bf16),
            pltpu.VMEM((8, 8, 48, ROWS), bf16),
            pltpu.VMEM((8, 16, TILE), f32),
            pltpu.VMEM((8, 16, TILE), f32),
            pltpu.VMEM((8, 24, TILE), f32),
            pltpu.VMEM((16, TILE), f32),
            pltpu.VMEM((4, 64, TILE), f32),
            pltpu.VMEM((2, 64, TILE), f32),
            pltpu.VMEM((16, TILE), f32),
            pltpu.VMEM((96, TILE), f32),
            dma((3,)), dma((3,)), dma((3,)), dma((3,)), dma,
            dma((UNITS,)), dma, dma,
            dma, dma, dma, dma,
            dma, dma, dma, dma, dma((7,)), dma, dma((7,)), dma, dma, dma,
            dma, dma((3,)),
        ],
        compiler_params=pltpu.CompilerParams(collective_id=0, has_side_effects=True, vmem_limit_bytes=48 * 2**20),
    )(wq, lq.T, hq, wk, lk.T, hk, wv, lv.T, hv, nt.reshape(1, -1), ns.reshape(1, -1))
    return (
        out[0].T, out[1].T, out[2].T,
        cols[0, :48], cols[1, :48], cols[2, :48],
        norm.reshape(-1),
    )


def solution(mesh):
    torus = Mesh(mesh.devices.reshape(8, 4, 2, 4), ("z", "y", "c", "x"))
    shard = ("z", "y", "c")
    in_specs = (P(shard, "x"), P(shard, None), P(None, "x")) * 3 + (P((*shard, "x")),) * 2
    columns = ("x", *shard)
    out_specs = (P(None, columns),) * 3 + (P(columns),) * 3 + (P(),)
    return jax.shard_map(body, mesh=torus, in_specs=in_specs, out_specs=out_specs, check_vma=False)
```

```python
import jax
import jax.numpy as jnp
from jax import lax
from jax.experimental import pallas as pl
from jax.experimental.pallas import tpu as pltpu
from jax.sharding import Mesh
from jax.sharding import PartitionSpec as P

D_MODEL = 12288
MIX_RATE = 0.5
MESH = pl.DeviceIdType.MESH
SIZES = {"z": 8, "y": 4, "c": 2, "x": 4}
ROWS = 192
TILE = 128
TILES = 9
UNITS = 36
Z_ORDER = (4, 3, 5, 2, 6, 1, 7)
PIECES = (
    ((0, 0, 0, 48), (1, 48, 0, 48), (2, 96, 0, 32)),
    ((2, 0, 32, 16), (3, 16, 0, 48), (4, 64, 0, 48), (5, 112, 0, 16)),
    ((5, 0, 16, 32), (6, 32, 0, 48), (7, 80, 0, 48)),
)
EARLY = 2


def shifted(**offsets):
    return {a: lax.rem(lax.axis_index(a) + o, SIZES[a]) for a, o in offsets.items()}


def all_peers():
    out = [{"z": dz, "c": dc} for dz in range(8) for dc in range(2) if dz or dc]
    out += [{"x": dx, "c": dc} for dx in range(1, 4) for dc in range(2)]
    out += [{"y": dy, "c": dc} for dy in range(1, 4) for dc in range(2)]
    return out


def remote(src, dst, send, recv, device):
    return pltpu.make_async_remote_copy(
        src_ref=src, dst_ref=dst, send_sem=send, recv_sem=recv, device_id=device, device_id_type=MESH
    )


def wait_bytes(ref, sem):
    pltpu.make_async_copy(ref, ref, sem).wait()


def product(low, high):
    return lax.dot_general(low, high, (((0,), (0,)), ((), ())), preferred_element_type=jnp.float32)


def kernel(
    wq, lq, hq, wk, lk, hk, wv, lv, hv, nt, ns,
    out, cols, norm,
    weights, highs, lows, units, ready, quarters, part, got1, got2, total, norms, gathered, mean, wide, gain,
    w_sem, h_sem, l_sem, q_sem, g_sem,
    unit_sem, z_send, c_send,
    low_send, low_recv, low_send2, low_recv2,
    s1_send, s1_recv, s2_send, s2_recv, s3_send, s3_recv, n3_send, n3_recv, n4_send, n4_recv,
    y_send, y_recv,
):
    z, y, c, x = (lax.axis_index(a) for a in ("z", "y", "c", "x"))
    member = 2 * y + c
    w_in, l_in, h_in = (wq, wk, wv), (lq, lk, lv), (hq, hk, hv)

    barrier = pltpu.get_barrier_semaphore()
    peers = all_peers()
    for p in peers:
        pl.semaphore_signal(barrier, inc=1, device_id=shifted(**p), device_id_type=MESH)

    loads = []
    for t in range(3):
        loads.append(
            (
                pltpu.make_async_copy(w_in[t], weights.at[t], w_sem.at[t]),
                pltpu.make_async_copy(h_in[t], highs.at[t], h_sem.at[t]),
                pltpu.make_async_copy(l_in[t], lows.at[t], l_sem.at[t]),
            )
        )
        for copy in loads[t]:
            copy.start()
    gain_loads = [pltpu.make_async_copy(ref, gain.at[n], g_sem.at[n]) for n, ref in enumerate((nt, ns))]
    for copy in gain_loads:
        copy.start()
    quarter = quarters.at[4 * c + x, 0]
    quarter_loads = []
    for t in range(3):
        copy = pltpu.make_async_copy(
            l_in[t].at[pl.ds(pl.multiple_of(16 * x, 16), 16), :],
            quarter.at[pl.ds(16 * t, 16), :],
            q_sem.at[t],
        )
        copy.start()
        quarter_loads.append(copy)

    def tile_of(turn):
        return lax.rem(turn + y, TILES)

    def slot_of(k, turn):
        return 4 * k + turn // 2 if turn < 8 else 32 + k // 2

    def half(slot, core):
        return units.at[pl.ds(pl.multiple_of(384 * slot + ROWS * core, 64), ROWS), :]

    def slab(k, turn):
        tile = tile_of(turn)
        first = 384 * lax.rem(z + k, 8) + TILE * (tile % 3)
        return weights.at[tile // 3, :, pl.ds(pl.multiple_of(first, TILE), TILE)]

    for turn in range(TILES):
        tile = tile_of(turn)
        first = 384 * z + TILE * (tile % 3)
        for t in range(3):

            @pl.when((c == turn % 2) & (tile // 3 == t))
            def _():
                slot = slot_of(0, turn)
                src = w_in[t].at[:, pl.ds(pl.multiple_of(first, TILE), TILE)]
                pltpu.make_async_copy(src, half(slot, c), unit_sem.at[slot]).start()

    pl.semaphore_wait(barrier, len(peers))
    for copy in quarter_loads:
        copy.wait()
    for t in range(3):
        loads[t][0].wait()

    for k in Z_ORDER:
        remote(quarter, quarters.at[4 * c + x, k], low_send, low_recv, shifted(z=k)).start()
    for turn in range(TILES):

        @pl.when(c != turn % 2)
        def _():
            slot = slot_of(0, turn)
            remote(slab(0, turn), half(slot, c), c_send, unit_sem.at[slot], shifted(c=1)).start()

    def send_round(turn):
        for k in Z_ORDER:
            slot = slot_of(k, turn)
            device = {"z": lax.rem(z + k, 8), "c": (k + turn) % 2}
            remote(slab(k, turn), half(slot, c), z_send, unit_sem.at[slot], device).start()


    for turn in range(EARLY):
        send_round(turn)

    for t in range(3):
        for copy in loads[t][1:]:
            copy.wait()
        low = lows[t]

        def sums(s, _):
            for j in range(3):
                first = pl.ds(pl.multiple_of(384 * s + TILE * j, TILE), TILE)
                latest = weights[t, :, first].astype(jnp.float32) + MIX_RATE * product(low, highs[t, :, first])
                part[s, pl.ds(3 * t + j, 1), :] = jnp.sum(jnp.abs(latest), axis=0, keepdims=True)
            return 0

        lax.fori_loop(0, 8, sums, 0)
    for copy in gain_loads:
        copy.wait()
    own_norm = jnp.concatenate([gain[0] + gain[1], jnp.zeros((1, 80), jnp.float32)], axis=1)
    for s in range(8):
        part[s, pl.ds(9, 1), :] = own_norm
    for dy in range(4):
        for dc in range(2):
            if dy or dc:
                to = shifted(y=dy, c=dc)
                remote(part.at[2 * to["y"] + to["c"]], got1.at[member], s1_send, s1_recv, to).start()
    got1[member] = part[member]
    wait_bytes(got1.at[pl.ds(0, 7)], s1_recv)
    mine = got1[0]
    for m in range(1, 8):
        mine = mine + got1[m]
    got2[0, pl.ds(0, 16), :] = mine
    for m in range(8):
        got2[0, pl.ds(16 + m, 1), :] = got1[m, pl.ds(9, 1), :]

    steps = lax.rem(member + 8 - z, 8)

    @pl.when(steps != 0)
    def _():
        remote(got2.at[0], got2.at[steps], s2_send, s2_recv, {"z": member}).start()

    for turn in range(EARLY, TILES):
        send_round(turn)

    wait_bytes(quarters.at[0, pl.ds(0, 7)], low_recv)
    for dx in range(4):
        for dc in range(2):
            if dx or dc:
                place = quarters.at[4 * c + x]
                remote(place, place, low_send2, low_recv2, shifted(x=dx, c=dc)).start()

    @pl.when(steps == 0)
    def _():
        wait_bytes(got2.at[pl.ds(0, 7)], s2_recv)
        whole = got2[0, pl.ds(0, 16), :]
        for k in range(1, 8):
            whole = whole + got2[k, pl.ds(0, 16), :]
        total[...] = whole
        for k in range(8):
            plane = lax.rem(z + 8 - k, 8)
            norms[x, pl.ds(pl.multiple_of(8 * plane, 8), 8), :] = got2[k, pl.ds(16, 8), :]
        for src, dst, send, recv in (
            (total, total, s3_send, s3_recv),
            (norms.at[x], norms.at[x], n3_send, n3_recv),
        ):
            n = 0
            for dy in range(4):
                for dc in range(2):
                    if dy or dc:
                        remote(src, dst, send.at[n], recv, shifted(y=dy, c=dc)).start()
                        n += 1

    @pl.when(steps != 0)
    def _():
        wait_bytes(total, s3_recv)
        wait_bytes(norms.at[x], n3_recv)

    for n, dx in enumerate((1, 2, 3)):
        remote(norms.at[x], norms.at[x], n4_send, n4_recv, shifted(x=dx)).start()
    mean[...] = total[...] / D_MODEL
    wait_bytes(quarters.at[pl.ds(0, 7)], low_recv2)

    own = 5 - c

    def unit(n):
        mine = n < own
        m = jnp.where(mine, 0, n - own)
        pair, place = m // 7, m % 7
        first = place < 3 + c
        index = jnp.where(first, place, place - 3 - c)
        turn = jnp.where(mine, 2 * n + c, 2 * pair + jnp.where(first, 0, 1))
        even = jnp.where(index == 0, 4, jnp.where(index == 1, 2, 6))
        odd = jnp.where(index == 0, 3, jnp.where(index == 1, 5, jnp.where(index == 2, 1, 7)))
        k = jnp.where(mine, 0, jnp.where((turn + c) % 2 == 0, even, odd))
        slot = jnp.where(turn == 8, 32 + k // 2, 4 * k + turn // 2)
        return k, tile_of(turn), slot

    def work(n):
        k, tile, slot = unit(n)
        tensor = tile // 3
        here = pl.ds(pl.multiple_of(384 * slot, 128), 384)
        wait_bytes(units.at[here, :], unit_sem.at[slot])
        first = 384 * z + TILE * (tile % 3)
        high = highs[tensor, :, pl.ds(pl.multiple_of(first, TILE), TILE)]
        rank = pl.ds(pl.multiple_of(16 * tensor, 16), 16)
        low = [
            jnp.concatenate([quarters[4 * core + q, k, rank, :] for q in range(4)], axis=0) for core in range(2)
        ]
        added = jnp.concatenate([product(a, high) for a in low], axis=0)
        latest = units[here, :].astype(jnp.float32) + MIX_RATE * added
        scaled = latest / mean[pl.ds(tile, 1), :]
        ready[pl.ds(pl.multiple_of(TILE * slot, TILE), TILE), :] = scaled.astype(jnp.bfloat16).T

    def hand_on(n):
        k, tile, slot = unit(n)
        tensor = tile // 3
        chip = 4 * lax.rem(z + 8 - k, 8) + y
        lanes = pl.ds(pl.multiple_of(384 * chip, 128), 384)
        for t in range(3):

            @pl.when(tile % 3 == t)
            def _():
                for owner, row, column, length in PIECES[t]:
                    src = ready.at[pl.ds(pl.multiple_of(TILE * slot + row, 16), length), :]
                    dst = out.at[tensor, pl.ds(column, length), lanes]

                    @pl.when(member == owner)
                    def _():
                        pltpu.make_async_copy(src, dst, y_recv.at[tensor]).start()

                    @pl.when(member != owner)
                    def _():
                        to = {"y": owner // 2, "c": owner % 2}
                        remote(src, dst, y_send, y_recv.at[tensor], to).start()

    def step(n, _):
        work(n)

        @pl.when(n > 0)
        def _():
            hand_on(n - 1)

        return 0

    lax.fori_loop(0, UNITS, step, 0)
    hand_on(UNITS - 1)

    for m in range(8):

        @pl.when(member == m)
        def _():
            for t in range(3):
                rows = [mean[pl.ds(3 * t + j, 1), :] for j in range(3)]
                line = jnp.concatenate(rows, axis=1)
                cols[pl.ds(t, 1), pl.ds(0, 48)] = line[:, 48 * m : 48 * m + 48]

    wait_bytes(norms.at[pl.ds(0, 3)], n4_recv)
    place = lax.broadcasted_iota(jnp.int32, (64, TILE), 1)
    n0, n1, n2, n3 = (norms[i] for i in range(4))
    r1, r2, r3 = pltpu.roll(n1, 48, 1), pltpu.roll(n2, 96, 1), pltpu.roll(n3, 16, 1)
    gathered[0] = jnp.where(place < 48, n0, jnp.where(place < 96, r1, r2))
    gathered[1] = jnp.where(place < 16, r2, r3)
    even, odd = pl.ds(0, 32, stride=2), pl.ds(1, 32, stride=2)
    a0, a1, b0, b1 = gathered[0, even, :], gathered[0, odd, :], gathered[1, even, :], gathered[1, odd, :]
    low_half = lax.broadcasted_iota(jnp.int32, (32, TILE), 1) < 64
    wide[pl.ds(0, 32, stride=3), :] = a0
    wide[pl.ds(1, 32, stride=3), :] = jnp.where(low_half, b0, pltpu.roll(a1, 64, 1))
    wide[pl.ds(2, 32, stride=3), :] = jnp.where(low_half, pltpu.roll(a1, 64, 1), pltpu.roll(b1, 64, 1))
    norm[...] = wide[...].astype(jnp.bfloat16)

    for t in range(3):
        wait_bytes(out.at[t], y_recv.at[t])
    wait_bytes(ready.at[pl.ds(0, 4032), :], y_send)
    wait_bytes(units.at[pl.ds(0, 63 * ROWS), :], z_send)

    @pl.when(c == 0)
    def _():
        wait_bytes(units.at[pl.ds(0, 4 * ROWS), :], c_send)

    @pl.when(c != 0)
    def _():
        wait_bytes(units.at[pl.ds(0, 5 * ROWS), :], c_send)

    wait_bytes(quarters.at[0, pl.ds(0, 7)], low_send)
    wait_bytes(quarters.at[pl.ds(0, 7)], low_send2)
    wait_bytes(got1.at[pl.ds(0, 7)], s1_send)
    wait_bytes(norms.at[pl.ds(0, 3)], n4_send)

    @pl.when(steps != 0)
    def _():
        wait_bytes(got2.at[0], s2_send)

    @pl.when(steps == 0)
    def _():
        for n in range(7):
            wait_bytes(total, s3_send.at[n])
            wait_bytes(norms.at[0], n3_send.at[n])


def body(wq, lq, hq, wk, lk, hk, wv, lv, hv, nt, ns):
    anywhere = pl.BlockSpec(memory_space=pltpu.HBM)
    local = pl.BlockSpec(memory_space=pltpu.VMEM)
    dma = pltpu.SemaphoreType.DMA
    bf16, f32 = jnp.bfloat16, jnp.float32
    out, cols, norm = pl.pallas_call(
        kernel,
        name="merge_and_place",
        out_shape=(
            jax.ShapeDtypeStruct((3, 48, D_MODEL), bf16),
            jax.ShapeDtypeStruct((8, TILE), f32),
            jax.ShapeDtypeStruct((96, TILE), bf16),
        ),
        in_specs=[anywhere] * 11,
        out_specs=(anywhere, local, local),
        scratch_shapes=[
            pltpu.VMEM((3, ROWS, 3072), bf16),
            pltpu.VMEM((3, 64, 3072), bf16),
            pltpu.VMEM((3, 64, ROWS), bf16),
            pltpu.VMEM((UNITS * 384, TILE), bf16),
            pltpu.VMEM((UNITS * TILE, 384), bf16),
            pltpu.VMEM((8, 8, 48, ROWS), bf16),
            pltpu.VMEM((8, 16, TILE), f32),
            pltpu.VMEM((8, 16, TILE), f32),
            pltpu.VMEM((8, 24, TILE), f32),
            pltpu.VMEM((16, TILE), f32),
            pltpu.VMEM((4, 64, TILE), f32),
            pltpu.VMEM((2, 64, TILE), f32),
            pltpu.VMEM((16, TILE), f32),
            pltpu.VMEM((96, TILE), f32),
            pltpu.VMEM((2, 1, 48), f32),
            dma((3,)), dma((3,)), dma((3,)), dma((3,)), dma((2,)),
            dma((UNITS,)), dma, dma,
            dma, dma, dma, dma,
            dma, dma, dma, dma, dma((7,)), dma, dma((7,)), dma, dma, dma,
            dma, dma((3,)),
        ],
        compiler_params=pltpu.CompilerParams(collective_id=0, has_side_effects=True, vmem_limit_bytes=48 * 2**20),
    )(*[pltpu.with_memory_space_constraint(a, pltpu.HBM) for a in (wq, lq.T, hq, wk, lk.T, hk, wv, lv.T, hv, nt.reshape(1, -1), ns.reshape(1, -1))])
    return (
        out[0].T, out[1].T, out[2].T,
        cols[0, :48], cols[1, :48], cols[2, :48],
        norm.reshape(-1),
    )


def solution(mesh):
    torus = Mesh(mesh.devices.reshape(8, 4, 2, 4), ("z", "y", "c", "x"))
    shard = ("z", "y", "c")
    in_specs = (P(shard, "x"), P(shard, None), P(None, "x")) * 3 + (P((*shard, "x")),) * 2
    columns = ("x", *shard)
    out_specs = (P(None, columns),) * 3 + (P(columns),) * 3 + (P(),)
    return jax.shard_map(body, mesh=torus, in_specs=in_specs, out_specs=out_specs, check_vma=False)
```

```python
import jax
import jax.numpy as jnp
from jax import lax
from jax.experimental import pallas as pl
from jax.experimental.pallas import tpu as pltpu
from jax.sharding import Mesh
from jax.sharding import PartitionSpec as P

D_MODEL = 12288
MIX_RATE = 0.5
MESH = pl.DeviceIdType.MESH
SIZES = {"z": 8, "y": 4, "c": 2, "x": 4}
ROWS = 192
TILE = 128
TILES = 9
UNITS = 36
Z_ORDER = (4, 3, 5, 2, 6, 1, 7)
PIECES = (
    ((0, 0, 0, 48), (1, 48, 0, 48), (2, 96, 0, 32)),
    ((2, 0, 32, 16), (3, 16, 0, 48), (4, 64, 0, 48), (5, 112, 0, 16)),
    ((5, 0, 16, 32), (6, 32, 0, 48), (7, 80, 0, 48)),
)


def shifted(**offsets):
    return {a: lax.rem(lax.axis_index(a) + o, SIZES[a]) for a, o in offsets.items()}


def all_peers():
    out = [{"z": dz, "c": dc} for dz in range(8) for dc in range(2) if dz or dc]
    out += [{"x": dx, "c": dc} for dx in range(1, 4) for dc in range(2)]
    out += [{"y": dy, "c": dc} for dy in range(1, 4) for dc in range(2)]
    return out


def remote(src, dst, send, recv, device):
    return pltpu.make_async_remote_copy(
        src_ref=src, dst_ref=dst, send_sem=send, recv_sem=recv, device_id=device, device_id_type=MESH
    )


def wait_bytes(ref, sem):
    pltpu.make_async_copy(ref, ref, sem).wait()


def product(low, high):
    return lax.dot_general(low, high, (((0,), (0,)), ((), ())), preferred_element_type=jnp.float32)


def kernel(
    wq, lq, hq, wk, lk, hk, wv, lv, hv, nt, ns,
    out, col_q, col_k, col_v, norm,
    weights, highs, lows, units, ready, quarters, part, got1, got2, total, norms, gathered, mean, wide, gain,
    w_sem, h_sem, l_sem, q_sem, g_sem,
    unit_sem, z_send, c_send,
    low_send, low_recv, low_send2, low_recv2, low_send3, low_recv3,
    s1_send, s1_recv, s2_send, s2_recv, s3_send, s3_recv, n3_send, n3_recv, n4_send, n4_recv,
    y_send, y_recv,
):
    z, y, c, x = (lax.axis_index(a) for a in ("z", "y", "c", "x"))
    member = 2 * y + c
    w_in, l_in, h_in = (wq, wk, wv), (lq, lk, lv), (hq, hk, hv)

    barrier = pltpu.get_barrier_semaphore()
    peers = all_peers()
    for p in peers:
        pl.semaphore_signal(barrier, inc=1, device_id=shifted(**p), device_id_type=MESH)

    loads = []
    for t in range(3):
        loads.append(
            (
                pltpu.make_async_copy(w_in[t], weights.at[t], w_sem.at[t]),
                pltpu.make_async_copy(h_in[t], highs.at[t], h_sem.at[t]),
                pltpu.make_async_copy(l_in[t], lows.at[t], l_sem.at[t]),
            )
        )
        for copy in loads[t]:
            copy.start()
    gain_loads = [pltpu.make_async_copy(ref, gain.at[n], g_sem.at[n]) for n, ref in enumerate((nt, ns))]
    for copy in gain_loads:
        copy.start()
    quarter = quarters.at[4 * c + x, 0]
    quarter_loads = []
    for t in range(3):
        copy = pltpu.make_async_copy(
            l_in[t].at[pl.ds(pl.multiple_of(16 * x, 16), 16), :],
            quarter.at[pl.ds(16 * t, 16), :],
            q_sem.at[t],
        )
        copy.start()
        quarter_loads.append(copy)

    def tile_of(turn):
        return 3 * (turn // 3) + ((y + 1) // 2 + 8 - turn) % 3

    def slot_of(k, turn):
        return 4 * k + turn // 2 if turn < 8 else 32 + k // 2

    def half(slot, core):
        return units.at[pl.ds(pl.multiple_of(384 * slot + ROWS * core, 64), ROWS), :]

    def slab(k, turn):
        first = 384 * lax.rem(z + k, 8) + TILE * (tile_of(turn) % 3)
        return weights.at[turn // 3, :, pl.ds(pl.multiple_of(first, TILE), TILE)]

    for turn in range(TILES):
        first = 384 * z + TILE * (tile_of(turn) % 3)

        @pl.when(c == turn % 2)
        def _():
            slot = slot_of(0, turn)
            src = w_in[turn // 3].at[:, pl.ds(pl.multiple_of(first, TILE), TILE)]
            pltpu.make_async_copy(src, half(slot, c), unit_sem.at[slot]).start()

    pl.semaphore_wait(barrier, len(peers))
    for copy in quarter_loads:
        copy.wait()
    for t in range(3):
        loads[t][0].wait()

    def pass_low(k, step):
        place = (k + step) % 8
        lane = 4 * c + x
        device = shifted(z=step % 8)
        remote(quarters.at[lane, k], quarters.at[lane, place], low_send, low_recv.at[place], device).start()

    def wait_low(k):
        wait_bytes(quarters.at[0, k], low_recv.at[k])

    def spread_low(*planes):
        for k in planes:
            place = quarters.at[4 * c + x, k]
            for dx in (1, 2, 3):
                remote(place, place, low_send2, low_recv2, shifted(x=dx)).start()

    pass_low(0, 1)
    pass_low(0, -1)
    for turn in range(TILES):

        @pl.when(c != turn % 2)
        def _():
            slot = slot_of(0, turn)
            remote(slab(0, turn), half(slot, c), c_send, unit_sem.at[slot], shifted(c=1)).start()

    def send_round(turn, order=Z_ORDER):
        for k in order:
            slot = slot_of(k, turn)
            device = {"z": lax.rem(z + k, 8), "c": (k + turn) % 2}
            remote(slab(k, turn), half(slot, c), z_send, unit_sem.at[slot], device).start()


    send_round(0, Z_ORDER[:3])
    wait_low(1)
    wait_low(7)
    pass_low(1, 1)
    pass_low(7, -1)
    send_round(0, Z_ORDER[3:])
    spread_low(0, 1, 7)

    def sum_up(t):
        low = lows[t]

        def sums(s, _):
            first = pl.ds(pl.multiple_of(384 * s, TILE), 384)
            latest = weights[t, :, first].astype(jnp.float32) + MIX_RATE * product(low[...], highs[t, :, first])
            line = jnp.sum(jnp.abs(latest), axis=0, keepdims=True)
            for j in range(3):
                part[s, pl.ds(3 * t + j, 1), :] = line[:, TILE * j : TILE * (j + 1)]
            return 0

        lax.fori_loop(0, 8, sums, 0)

    for t in range(3):
        for copy in loads[t][1:]:
            copy.wait()
    for copy in gain_loads:
        copy.wait()
    own_norm = jnp.concatenate([gain[0] + gain[1], jnp.zeros((1, 80), jnp.float32)], axis=1)
    for s in range(8):
        part[s, pl.ds(9, 1), :] = own_norm
    sum_up(0)

    wait_low(2)
    wait_low(6)
    pass_low(2, 1)
    pass_low(6, -1)
    send_round(1, Z_ORDER[:3])
    spread_low(2, 6)

    sum_up(1)

    wait_low(3)
    wait_low(5)

    @pl.when(z % 2 == 1)
    def _():
        pass_low(3, 1)

    @pl.when(z % 2 == 0)
    def _():
        pass_low(5, -1)

    send_round(1, Z_ORDER[3:])
    spread_low(3, 5)

    sum_up(2)

    for dy in range(4):
        for dc in range(2):
            if dy or dc:
                to = shifted(y=dy, c=dc)
                remote(part.at[2 * to["y"] + to["c"]], got1.at[member], s1_send, s1_recv, to).start()
    got1[member] = part[member]
    send_round(2, Z_ORDER[:2])
    wait_bytes(got1.at[pl.ds(0, 7)], s1_recv)
    mine = got1[0]
    for m in range(1, 8):
        mine = mine + got1[m]
    got2[0, pl.ds(0, 16), :] = mine
    for m in range(8):
        got2[0, pl.ds(16 + m, 1), :] = got1[m, pl.ds(9, 1), :]

    steps = lax.rem(member + 8 - z, 8)

    @pl.when(steps != 0)
    def _():
        remote(got2.at[0], got2.at[steps], s2_send, s2_recv, {"z": member}).start()

    wait_low(4)
    spread_low(4)
    send_round(2, Z_ORDER[2:])
    for turn in range(3, TILES):
        send_round(turn)

    wait_bytes(quarters.at[pl.ds(0, 3)], low_recv2)
    half_low = quarters.at[pl.ds(4 * c, 4)]
    remote(half_low, half_low, low_send3, low_recv3, shifted(c=1)).start()

    @pl.when(steps == 0)
    def _():
        wait_bytes(got2.at[pl.ds(0, 7)], s2_recv)
        whole = got2[0, pl.ds(0, 16), :]
        for k in range(1, 8):
            whole = whole + got2[k, pl.ds(0, 16), :]
        total[...] = whole
        for k in range(8):
            plane = lax.rem(z + 8 - k, 8)
            norms[x, pl.ds(pl.multiple_of(8 * plane, 8), 8), :] = got2[k, pl.ds(16, 8), :]
        for src, dst, send, recv in (
            (total, total, s3_send, s3_recv),
            (norms.at[x], norms.at[x], n3_send, n3_recv),
        ):
            n = 0
            for dy in range(4):
                for dc in range(2):
                    if dy or dc:
                        remote(src, dst, send.at[n], recv, shifted(y=dy, c=dc)).start()
                        n += 1

    @pl.when(steps != 0)
    def _():
        wait_bytes(total, s3_recv)
        wait_bytes(norms.at[x], n3_recv)

    for n, dx in enumerate((1, 2, 3)):
        remote(norms.at[x], norms.at[x], n4_send, n4_recv, shifted(x=dx)).start()
    mean[...] = total[...] / D_MODEL
    wait_bytes(quarters.at[pl.ds(0, 4)], low_recv3)

    own = 5 - c

    def unit(n):
        mine = n < own
        m = jnp.where(mine, 0, n - own)
        pair, place = m // 7, m % 7
        first = place < 3 + c
        index = jnp.where(first, place, place - 3 - c)
        turn = jnp.where(mine, 2 * n + c, 2 * pair + jnp.where(first, 0, 1))
        even = jnp.where(index == 0, 4, jnp.where(index == 1, 2, 6))
        odd = jnp.where(index == 0, 3, jnp.where(index == 1, 5, jnp.where(index == 2, 1, 7)))
        k = jnp.where(mine, 0, jnp.where((turn + c) % 2 == 0, even, odd))
        slot = jnp.where(turn == 8, 32 + k // 2, 4 * k + turn // 2)
        return k, tile_of(turn), slot

    def work(n):
        k, tile, slot = unit(n)
        tensor = tile // 3
        here = pl.ds(pl.multiple_of(384 * slot, 128), 384)
        wait_bytes(units.at[here, :], unit_sem.at[slot])
        first = 384 * z + TILE * (tile % 3)
        high = highs[tensor, :, pl.ds(pl.multiple_of(first, TILE), TILE)]
        rank = pl.ds(pl.multiple_of(16 * tensor, 16), 16)
        low = [
            jnp.concatenate([quarters[4 * core + q, k, rank, :] for q in range(4)], axis=0) for core in range(2)
        ]
        added = jnp.concatenate([product(a, high) for a in low], axis=0)
        latest = units[here, :].astype(jnp.float32) + MIX_RATE * added
        scaled = latest / mean[pl.ds(tile, 1), :]
        ready[pl.ds(pl.multiple_of(TILE * slot, TILE), TILE), :] = scaled.astype(jnp.bfloat16).T

    def hand_on(n):
        k, tile, slot = unit(n)
        tensor = tile // 3
        chip = 4 * lax.rem(z + 8 - k, 8) + y
        lanes = pl.ds(pl.multiple_of(384 * chip, 128), 384)
        for t in range(3):

            @pl.when(tile % 3 == t)
            def _():
                for owner, row, column, length in PIECES[t]:
                    src = ready.at[pl.ds(pl.multiple_of(TILE * slot + row, 16), length), :]
                    dst = out.at[tensor, pl.ds(column, length), lanes]

                    @pl.when(member == owner)
                    def _():
                        pltpu.make_async_copy(src, dst, y_recv.at[tensor]).start()

                    @pl.when(member != owner)
                    def _():
                        to = {"y": owner // 2, "c": owner % 2}
                        remote(src, dst, y_send, y_recv.at[tensor], to).start()

    def step(n, _):
        work(n)

        @pl.when(n > 0)
        def _():
            hand_on(n - 1)

        return 0

    lax.fori_loop(0, UNITS, step, 0)
    hand_on(UNITS - 1)

    for m in range(8):

        @pl.when(member == m)
        def _():
            for t in range(3):
                rows = [mean[pl.ds(3 * t + j, 1), :] for j in range(3)]
                line = jnp.concatenate(rows, axis=1)
                (col_q, col_k, col_v)[t][...] = line[:, 48 * m : 48 * m + 48]

    wait_bytes(norms.at[pl.ds(0, 3)], n4_recv)
    place = lax.broadcasted_iota(jnp.int32, (64, TILE), 1)
    n0, n1, n2, n3 = (norms[i] for i in range(4))
    r1, r2, r3 = pltpu.roll(n1, 48, 1), pltpu.roll(n2, 96, 1), pltpu.roll(n3, 16, 1)
    gathered[0] = jnp.where(place < 48, n0, jnp.where(place < 96, r1, r2))
    gathered[1] = jnp.where(place < 16, r2, r3)
    even, odd = pl.ds(0, 32, stride=2), pl.ds(1, 32, stride=2)
    a0, a1, b0, b1 = gathered[0, even, :], gathered[0, odd, :], gathered[1, even, :], gathered[1, odd, :]
    low_half = lax.broadcasted_iota(jnp.int32, (32, TILE), 1) < 64
    wide[pl.ds(0, 32, stride=3), :] = a0
    wide[pl.ds(1, 32, stride=3), :] = jnp.where(low_half, b0, pltpu.roll(a1, 64, 1))
    wide[pl.ds(2, 32, stride=3), :] = jnp.where(low_half, pltpu.roll(a1, 64, 1), pltpu.roll(b1, 64, 1))
    norm[...] = wide[...].astype(jnp.bfloat16)

    for t in range(3):
        wait_bytes(out.at[t], y_recv.at[t])
    wait_bytes(ready.at[pl.ds(0, 4032), :], y_send)
    wait_bytes(units.at[pl.ds(0, 63 * ROWS), :], z_send)

    @pl.when(c == 0)
    def _():
        wait_bytes(units.at[pl.ds(0, 4 * ROWS), :], c_send)

    @pl.when(c != 0)
    def _():
        wait_bytes(units.at[pl.ds(0, 5 * ROWS), :], c_send)

    wait_bytes(quarters.at[0, pl.ds(0, 7)], low_send)
    wait_bytes(quarters.at[pl.ds(0, 3)], low_send2)
    wait_bytes(quarters.at[pl.ds(0, 4)], low_send3)
    wait_bytes(got1.at[pl.ds(0, 7)], s1_send)
    wait_bytes(norms.at[pl.ds(0, 3)], n4_send)

    @pl.when(steps != 0)
    def _():
        wait_bytes(got2.at[0], s2_send)

    @pl.when(steps == 0)
    def _():
        for n in range(7):
            wait_bytes(total, s3_send.at[n])
            wait_bytes(norms.at[0], n3_send.at[n])


def settle(out, cq, ck, cv, norm, *results):
    *to, sem = results
    copies = [
        pltpu.make_async_copy(src, dst, sem.at[n])
        for n, (src, dst) in enumerate(zip((out.at[0], out.at[1], out.at[2], cq, ck, cv, norm), to))
    ]
    for copy in copies:
        copy.start()
    for copy in copies:
        copy.wait()


def body(wq, lq, hq, wk, lk, hk, wv, lv, hv, nt, ns):
    anywhere = pl.BlockSpec(memory_space=pltpu.HBM)
    local = pl.BlockSpec(memory_space=pltpu.VMEM)
    dma = pltpu.SemaphoreType.DMA
    bf16, f32 = jnp.bfloat16, jnp.float32
    out, *small = pl.pallas_call(
        kernel,
        name="merge_and_place",
        out_shape=(
            jax.ShapeDtypeStruct((3, 48, D_MODEL), bf16),
            *[jax.ShapeDtypeStruct((1, 48), f32)] * 3,
            jax.ShapeDtypeStruct((96, TILE), bf16),
        ),
        in_specs=[anywhere] * 11,
        out_specs=(anywhere, local, local, local, local),
        scratch_shapes=[
            pltpu.VMEM((3, ROWS, 3072), bf16),
            pltpu.VMEM((3, 64, 3072), bf16),
            pltpu.VMEM((3, 64, ROWS), bf16),
            pltpu.VMEM((UNITS * 384, TILE), bf16),
            pltpu.VMEM((UNITS * TILE, 384), bf16),
            pltpu.VMEM((8, 8, 48, ROWS), bf16),
            pltpu.VMEM((8, 16, TILE), f32),
            pltpu.VMEM((8, 16, TILE), f32),
            pltpu.VMEM((8, 24, TILE), f32),
            pltpu.VMEM((16, TILE), f32),
            pltpu.VMEM((4, 64, TILE), f32),
            pltpu.VMEM((2, 64, TILE), f32),
            pltpu.VMEM((16, TILE), f32),
            pltpu.VMEM((96, TILE), f32),
            pltpu.VMEM((2, 1, 48), f32),
            dma((3,)), dma((3,)), dma((3,)), dma((3,)), dma((2,)),
            dma((UNITS,)), dma, dma,
            dma, dma((8,)), dma, dma, dma, dma,
            dma, dma, dma, dma, dma((7,)), dma, dma((7,)), dma, dma, dma,
            dma, dma((3,)),
        ],
        compiler_params=pltpu.CompilerParams(collective_id=0, has_side_effects=True, vmem_limit_bytes=48 * 2**20),
    )(*[pltpu.with_memory_space_constraint(a, pltpu.HBM) for a in (wq, lq.T, hq, wk, lk.T, hk, wv, lv.T, hv, nt.reshape(1, -1), ns.reshape(1, -1))])
    either = pl.BlockSpec(memory_space=pl.ANY)
    q, k, v, cq, ck, cv, norm = pl.pallas_call(
        settle,
        name="settle",
        out_shape=(
            *[jax.ShapeDtypeStruct((48, D_MODEL), bf16)] * 3,
            *[jax.ShapeDtypeStruct((1, 48), f32)] * 3,
            jax.ShapeDtypeStruct((96, TILE), bf16),
        ),
        in_specs=[either] * 5,
        out_specs=[either] * 7,
        scratch_shapes=[dma((7,))],
        compiler_params=pltpu.CompilerParams(vmem_limit_bytes=2**20),
    )(out, *small)
    return q.T, k.T, v.T, cq.reshape(-1), ck.reshape(-1), cv.reshape(-1), norm.reshape(-1)


def solution(mesh):
    torus = Mesh(mesh.devices.reshape(8, 4, 2, 4), ("z", "y", "c", "x"))
    shard = ("z", "y", "c")
    in_specs = (P(shard, "x"), P(shard, None), P(None, "x")) * 3 + (P((*shard, "x")),) * 2
    columns = ("x", *shard)
    out_specs = (P(None, columns),) * 3 + (P(columns),) * 3 + (P(),)
    return jax.shard_map(body, mesh=torus, in_specs=in_specs, out_specs=out_specs, check_vma=False)
```

```python
import jax
import jax.numpy as jnp
from jax import lax
from jax.experimental import pallas as pl
from jax.experimental.pallas import tpu as pltpu
from jax.sharding import Mesh
from jax.sharding import PartitionSpec as P

D_MODEL = 12288
MIX_RATE = 0.5
MESH = pl.DeviceIdType.MESH
SIZES = {"z": 8, "y": 4, "c": 2, "x": 4}
ROWS = 192
TILE = 128
TILES = 9
UNITS = 36
Z_ORDER = (1, 7, 3, 5, 2, 6, 4)
PIECES = (
    ((0, 0, 0, 48), (1, 48, 0, 48), (2, 96, 0, 32)),
    ((2, 0, 32, 16), (3, 16, 0, 48), (4, 64, 0, 48), (5, 112, 0, 16)),
    ((5, 0, 16, 32), (6, 32, 0, 48), (7, 80, 0, 48)),
)


def shifted(**offsets):
    return {a: lax.rem(lax.axis_index(a) + o, SIZES[a]) for a, o in offsets.items()}


def all_peers():
    out = [{"z": dz, "c": dc} for dz in range(8) for dc in range(2) if dz or dc]
    out += [{"x": dx, "c": dc} for dx in range(1, 4) for dc in range(2)]
    out += [{"y": dy, "c": dc} for dy in range(1, 4) for dc in range(2)]
    return out


def remote(src, dst, send, recv, device):
    return pltpu.make_async_remote_copy(
        src_ref=src, dst_ref=dst, send_sem=send, recv_sem=recv, device_id=device, device_id_type=MESH
    )


def wait_bytes(ref, sem):
    pltpu.make_async_copy(ref, ref, sem).wait()


def product(low, high):
    return lax.dot_general(low, high, (((0,), (0,)), ((), ())), preferred_element_type=jnp.float32)


def kernel(
    wq, lq, hq, wk, lk, hk, wv, lv, hv, nt, ns,
    out, col_q, col_k, col_v, norm,
    weights, highs, lows, units, ready, quarters, part, got1, got2, total, norms, gathered, mean, wide, gain,
    w_sem, h_sem, l_sem, q_sem, g_sem,
    unit_sem, z_send, c_send,
    low_send, low_recv, low_send2, low_recv2, low_send3, low_recv3,
    s1_send, s1_recv, s2_send, s2_recv, s3_send, s3_recv, n3_send, n3_recv, n4_send, n4_recv,
    y_send, y_recv,
):
    z, y, c, x = (lax.axis_index(a) for a in ("z", "y", "c", "x"))
    member = 2 * y + c
    w_in, l_in, h_in = (wq, wk, wv), (lq, lk, lv), (hq, hk, hv)

    barrier = pltpu.get_barrier_semaphore()
    peers = all_peers()
    for p in peers:
        pl.semaphore_signal(barrier, inc=1, device_id=shifted(**p), device_id_type=MESH)

    loads = []
    for t in range(3):
        loads.append(
            (
                pltpu.make_async_copy(w_in[t], weights.at[t], w_sem.at[t]),
                pltpu.make_async_copy(h_in[t], highs.at[t], h_sem.at[t]),
                pltpu.make_async_copy(l_in[t], lows.at[t], l_sem.at[t]),
            )
        )
        for copy in loads[t]:
            copy.start()
    gain_loads = [pltpu.make_async_copy(ref, gain.at[n], g_sem.at[n]) for n, ref in enumerate((nt, ns))]
    for copy in gain_loads:
        copy.start()
    quarter = quarters.at[4 * c + x, 0]
    quarter_loads = []
    for t in range(3):
        copy = pltpu.make_async_copy(
            l_in[t].at[pl.ds(pl.multiple_of(16 * x, 16), 16), :],
            quarter.at[pl.ds(16 * t, 16), :],
            q_sem.at[t],
        )
        copy.start()
        quarter_loads.append(copy)

    def tile_of(turn):
        return 3 * (turn // 3) + ((y + 1) // 2 + 8 - turn) % 3

    def slot_of(k, turn):
        return 4 * k + turn // 2 if turn < 8 else 32 + k // 2

    def half(slot, core):
        return units.at[pl.ds(pl.multiple_of(384 * slot + ROWS * core, 64), ROWS), :]

    def slab(k, turn):
        first = 384 * lax.rem(z + k, 8) + TILE * (tile_of(turn) % 3)
        return weights.at[turn // 3, :, pl.ds(pl.multiple_of(first, TILE), TILE)]

    for turn in range(TILES):
        first = 384 * z + TILE * (tile_of(turn) % 3)

        @pl.when(c == turn % 2)
        def _():
            slot = slot_of(0, turn)
            src = w_in[turn // 3].at[:, pl.ds(pl.multiple_of(first, TILE), TILE)]
            pltpu.make_async_copy(src, half(slot, c), unit_sem.at[slot]).start()

    pl.semaphore_wait(barrier, len(peers))
    for copy in quarter_loads:
        copy.wait()
    for t in range(3):
        loads[t][0].wait()

    def pass_low(k, step):
        place = (k + step) % 8
        lane = 4 * c + x
        device = shifted(z=step % 8)
        remote(quarters.at[lane, k], quarters.at[lane, place], low_send, low_recv.at[place], device).start()

    def wait_low(k):
        wait_bytes(quarters.at[0, k], low_recv.at[k])

    def spread_low(*planes):
        for k in planes:
            place = quarters.at[4 * c + x, k]
            for dx in (1, 2, 3):
                remote(place, place, low_send2, low_recv2, shifted(x=dx)).start()

    pass_low(0, 1)
    pass_low(0, -1)
    for turn in range(TILES):

        @pl.when(c != turn % 2)
        def _():
            slot = slot_of(0, turn)
            remote(slab(0, turn), half(slot, c), c_send, unit_sem.at[slot], shifted(c=1)).start()

    def send_round(turn, order=Z_ORDER):
        for k in order:
            slot = slot_of(k, turn)
            device = {"z": lax.rem(z + k, 8), "c": (k + k // 4 + turn) % 2}
            remote(slab(k, turn), half(slot, c), z_send, unit_sem.at[slot], device).start()


    send_round(0, Z_ORDER[:4])
    wait_low(1)
    wait_low(7)
    pass_low(1, 1)
    pass_low(7, -1)
    send_round(0, Z_ORDER[4:])
    spread_low(0, 1, 7)

    def sum_up(t):
        low = lows[t]

        def sums(s, _):
            first = pl.ds(pl.multiple_of(384 * s, TILE), 384)
            latest = weights[t, :, first].astype(jnp.float32) + MIX_RATE * product(low[...], highs[t, :, first])
            line = jnp.sum(jnp.abs(latest), axis=0, keepdims=True)
            for j in range(3):
                part[s, pl.ds(3 * t + j, 1), :] = line[:, TILE * j : TILE * (j + 1)]
            return 0

        lax.fori_loop(0, 8, sums, 0)

    for t in range(3):
        for copy in loads[t][1:]:
            copy.wait()
    for copy in gain_loads:
        copy.wait()
    own_norm = jnp.concatenate([gain[0] + gain[1], jnp.zeros((1, 80), jnp.float32)], axis=1)
    for s in range(8):
        part[s, pl.ds(9, 1), :] = own_norm
    sum_up(0)

    sum_up(1)
    sum_up(2)

    for dy in range(4):
        for dc in range(2):
            if dy or dc:
                to = shifted(y=dy, c=dc)
                remote(part.at[2 * to["y"] + to["c"]], got1.at[member], s1_send, s1_recv, to).start()

    wait_low(2)
    wait_low(6)
    pass_low(2, 1)
    pass_low(6, -1)
    send_round(1, Z_ORDER[:4])
    spread_low(2, 6)

    got1[member] = part[member]
    wait_bytes(got1.at[pl.ds(0, 7)], s1_recv)
    mine = got1[0]
    for m in range(1, 8):
        mine = mine + got1[m]
    got2[0, pl.ds(0, 16), :] = mine
    for m in range(8):
        got2[0, pl.ds(16 + m, 1), :] = got1[m, pl.ds(9, 1), :]

    steps = lax.rem(member + 8 - z, 8)

    @pl.when(steps != 0)
    def _():
        remote(got2.at[0], got2.at[steps], s2_send, s2_recv, {"z": member}).start()

    send_round(1, Z_ORDER[4:])
    wait_low(3)
    wait_low(5)

    @pl.when(z % 2 == 1)
    def _():
        pass_low(3, 1)

    @pl.when(z % 2 == 0)
    def _():
        pass_low(5, -1)

    for turn in range(2, TILES):
        send_round(turn)
    spread_low(3, 5)
    wait_low(4)
    spread_low(4)

    wait_bytes(quarters.at[pl.ds(0, 3)], low_recv2)
    half_low = quarters.at[pl.ds(4 * c, 4)]
    remote(half_low, half_low, low_send3, low_recv3, shifted(c=1)).start()

    @pl.when(steps == 0)
    def _():
        wait_bytes(got2.at[pl.ds(0, 7)], s2_recv)
        whole = got2[0, pl.ds(0, 16), :]
        for k in range(1, 8):
            whole = whole + got2[k, pl.ds(0, 16), :]
        total[...] = whole
        for k in range(8):
            plane = lax.rem(z + 8 - k, 8)
            norms[x, pl.ds(pl.multiple_of(8 * plane, 8), 8), :] = got2[k, pl.ds(16, 8), :]
        for src, dst, send, recv in (
            (total, total, s3_send, s3_recv),
            (norms.at[x], norms.at[x], n3_send, n3_recv),
        ):
            n = 0
            for dy in range(4):
                for dc in range(2):
                    if dy or dc:
                        remote(src, dst, send.at[n], recv, shifted(y=dy, c=dc)).start()
                        n += 1

    @pl.when(steps != 0)
    def _():
        wait_bytes(total, s3_recv)
        wait_bytes(norms.at[x], n3_recv)

    for n, dx in enumerate((1, 2, 3)):
        remote(norms.at[x], norms.at[x], n4_send, n4_recv, shifted(x=dx)).start()
    mean[...] = total[...] / D_MODEL
    wait_bytes(quarters.at[pl.ds(0, 4)], low_recv3)

    own = 5 - c

    def unit(n):
        mine = n < own
        m = jnp.where(mine, 0, n - own)
        pair, place = m // 7, m % 7
        first = place < 3 + c
        index = jnp.where(first, place, place - 3 - c)
        turn = jnp.where(mine, 2 * n + c, 2 * pair + jnp.where(first, 0, 1))
        one = jnp.where(index == 0, 7, jnp.where(index == 1, 5, 2))
        other = jnp.where(index == 0, 1, jnp.where(index == 1, 3, jnp.where(index == 2, 6, 4)))
        k = jnp.where(mine, 0, jnp.where((turn + c) % 2 == 0, one, other))
        slot = jnp.where(turn == 8, 32 + k // 2, 4 * k + turn // 2)
        return k, tile_of(turn), slot

    def work(n):
        k, tile, slot = unit(n)
        tensor = tile // 3
        here = pl.ds(pl.multiple_of(384 * slot, 128), 384)
        wait_bytes(units.at[here, :], unit_sem.at[slot])
        first = 384 * z + TILE * (tile % 3)
        high = highs[tensor, :, pl.ds(pl.multiple_of(first, TILE), TILE)]
        rank = pl.ds(pl.multiple_of(16 * tensor, 16), 16)
        low = [
            jnp.concatenate([quarters[4 * core + q, k, rank, :] for q in range(4)], axis=0) for core in range(2)
        ]
        added = jnp.concatenate([product(a, high) for a in low], axis=0)
        latest = units[here, :].astype(jnp.float32) + MIX_RATE * added
        scaled = latest / mean[pl.ds(tile, 1), :]
        ready[pl.ds(pl.multiple_of(TILE * slot, TILE), TILE), :] = scaled.astype(jnp.bfloat16).T

    def hand_on(n):
        k, tile, slot = unit(n)
        tensor = tile // 3
        chip = 4 * lax.rem(z + 8 - k, 8) + y
        lanes = pl.ds(pl.multiple_of(384 * chip, 128), 384)
        for t in range(3):

            @pl.when(tile % 3 == t)
            def _():
                for owner, row, column, length in PIECES[t]:
                    src = ready.at[pl.ds(pl.multiple_of(TILE * slot + row, 16), length), :]
                    dst = out.at[tensor, pl.ds(column, length), lanes]

                    @pl.when(member == owner)
                    def _():
                        pltpu.make_async_copy(src, dst, y_recv.at[tensor]).start()

                    @pl.when(member != owner)
                    def _():
                        to = {"y": owner // 2, "c": owner % 2}
                        remote(src, dst, y_send, y_recv.at[tensor], to).start()

    def step(n, _):
        work(n)

        @pl.when(n > 0)
        def _():
            hand_on(n - 1)

        return 0

    lax.fori_loop(0, UNITS, step, 0)
    hand_on(UNITS - 1)

    for m in range(8):

        @pl.when(member == m)
        def _():
            for t in range(3):
                rows = [mean[pl.ds(3 * t + j, 1), :] for j in range(3)]
                line = jnp.concatenate(rows, axis=1)
                (col_q, col_k, col_v)[t][...] = line[:, 48 * m : 48 * m + 48]

    wait_bytes(norms.at[pl.ds(0, 3)], n4_recv)
    place = lax.broadcasted_iota(jnp.int32, (64, TILE), 1)
    n0, n1, n2, n3 = (norms[i] for i in range(4))
    r1, r2, r3 = pltpu.roll(n1, 48, 1), pltpu.roll(n2, 96, 1), pltpu.roll(n3, 16, 1)
    gathered[0] = jnp.where(place < 48, n0, jnp.where(place < 96, r1, r2))
    gathered[1] = jnp.where(place < 16, r2, r3)
    even, odd = pl.ds(0, 32, stride=2), pl.ds(1, 32, stride=2)
    a0, a1, b0, b1 = gathered[0, even, :], gathered[0, odd, :], gathered[1, even, :], gathered[1, odd, :]
    low_half = lax.broadcasted_iota(jnp.int32, (32, TILE), 1) < 64
    wide[pl.ds(0, 32, stride=3), :] = a0
    wide[pl.ds(1, 32, stride=3), :] = jnp.where(low_half, b0, pltpu.roll(a1, 64, 1))
    wide[pl.ds(2, 32, stride=3), :] = jnp.where(low_half, pltpu.roll(a1, 64, 1), pltpu.roll(b1, 64, 1))
    norm[...] = wide[...].astype(jnp.bfloat16)

    for t in range(3):
        wait_bytes(out.at[t], y_recv.at[t])
    wait_bytes(ready.at[pl.ds(0, 4032), :], y_send)
    wait_bytes(units.at[pl.ds(0, 63 * ROWS), :], z_send)

    @pl.when(c == 0)
    def _():
        wait_bytes(units.at[pl.ds(0, 4 * ROWS), :], c_send)

    @pl.when(c != 0)
    def _():
        wait_bytes(units.at[pl.ds(0, 5 * ROWS), :], c_send)

    wait_bytes(quarters.at[0, pl.ds(0, 7)], low_send)
    wait_bytes(quarters.at[pl.ds(0, 3)], low_send2)
    wait_bytes(quarters.at[pl.ds(0, 4)], low_send3)
    wait_bytes(got1.at[pl.ds(0, 7)], s1_send)
    wait_bytes(norms.at[pl.ds(0, 3)], n4_send)

    @pl.when(steps != 0)
    def _():
        wait_bytes(got2.at[0], s2_send)

    @pl.when(steps == 0)
    def _():
        for n in range(7):
            wait_bytes(total, s3_send.at[n])
            wait_bytes(norms.at[0], n3_send.at[n])


def settle(out, cq, ck, cv, norm, *results):
    *to, sem = results
    copies = [
        pltpu.make_async_copy(src, dst, sem.at[n])
        for n, (src, dst) in enumerate(zip((out.at[0], out.at[1], out.at[2], cq, ck, cv, norm), to))
    ]
    for copy in copies:
        copy.start()
    for copy in copies:
        copy.wait()


def body(wq, lq, hq, wk, lk, hk, wv, lv, hv, nt, ns):
    anywhere = pl.BlockSpec(memory_space=pltpu.HBM)
    local = pl.BlockSpec(memory_space=pltpu.VMEM)
    dma = pltpu.SemaphoreType.DMA
    bf16, f32 = jnp.bfloat16, jnp.float32
    out, *small = pl.pallas_call(
        kernel,
        name="merge_and_place",
        out_shape=(
            jax.ShapeDtypeStruct((3, 48, D_MODEL), bf16),
            *[jax.ShapeDtypeStruct((1, 48), f32)] * 3,
            jax.ShapeDtypeStruct((96, TILE), bf16),
        ),
        in_specs=[anywhere] * 11,
        out_specs=(anywhere, local, local, local, local),
        scratch_shapes=[
            pltpu.VMEM((3, ROWS, 3072), bf16),
            pltpu.VMEM((3, 64, 3072), bf16),
            pltpu.VMEM((3, 64, ROWS), bf16),
            pltpu.VMEM((UNITS * 384, TILE), bf16),
            pltpu.VMEM((UNITS * TILE, 384), bf16),
            pltpu.VMEM((8, 8, 48, ROWS), bf16),
            pltpu.VMEM((8, 16, TILE), f32),
            pltpu.VMEM((8, 16, TILE), f32),
            pltpu.VMEM((8, 24, TILE), f32),
            pltpu.VMEM((16, TILE), f32),
            pltpu.VMEM((4, 64, TILE), f32),
            pltpu.VMEM((2, 64, TILE), f32),
            pltpu.VMEM((16, TILE), f32),
            pltpu.VMEM((96, TILE), f32),
            pltpu.VMEM((2, 1, 48), f32),
            dma((3,)), dma((3,)), dma((3,)), dma((3,)), dma((2,)),
            dma((UNITS,)), dma, dma,
            dma, dma((8,)), dma, dma, dma, dma,
            dma, dma, dma, dma, dma((7,)), dma, dma((7,)), dma, dma, dma,
            dma, dma((3,)),
        ],
        compiler_params=pltpu.CompilerParams(collective_id=0, has_side_effects=True, vmem_limit_bytes=48 * 2**20),
    )(*[pltpu.with_memory_space_constraint(a, pltpu.HBM) for a in (wq, lq.T, hq, wk, lk.T, hk, wv, lv.T, hv, nt.reshape(1, -1), ns.reshape(1, -1))])
    either = pl.BlockSpec(memory_space=pl.ANY)
    q, k, v, cq, ck, cv, norm = pl.pallas_call(
        settle,
        name="settle",
        out_shape=(
            *[jax.ShapeDtypeStruct((48, D_MODEL), bf16)] * 3,
            *[jax.ShapeDtypeStruct((1, 48), f32)] * 3,
            jax.ShapeDtypeStruct((96, TILE), bf16),
        ),
        in_specs=[either] * 5,
        out_specs=[either] * 7,
        scratch_shapes=[dma((7,))],
        compiler_params=pltpu.CompilerParams(vmem_limit_bytes=2**20),
    )(out, *small)
    return q.T, k.T, v.T, cq.reshape(-1), ck.reshape(-1), cv.reshape(-1), norm.reshape(-1)


def solution(mesh):
    torus = Mesh(mesh.devices.reshape(8, 4, 2, 4), ("z", "y", "c", "x"))
    shard = ("z", "y", "c")
    in_specs = (P(shard, "x"), P(shard, None), P(None, "x")) * 3 + (P((*shard, "x")),) * 2
    columns = ("x", *shard)
    out_specs = (P(None, columns),) * 3 + (P(columns),) * 3 + (P(),)
    return jax.shard_map(body, mesh=torus, in_specs=in_specs, out_specs=out_specs, check_vma=False)
```

```python
import jax
import jax.numpy as jnp
from jax import lax
from jax.experimental import pallas as pl
from jax.experimental.pallas import tpu as pltpu
from jax.sharding import Mesh
from jax.sharding import PartitionSpec as P

D_MODEL = 12288
MIX_RATE = 0.5
MESH = pl.DeviceIdType.MESH
SIZES = {"z": 8, "y": 4, "c": 2, "x": 4}
ROWS = 192
TILE = 128
TILES = 9
UNITS = 36
Z_ORDER = (2, 6, 3, 5, 1, 7, 4)
PIECES = (
    ((0, 0, 0, 48), (1, 48, 0, 48), (2, 96, 0, 32)),
    ((2, 0, 32, 16), (3, 16, 0, 48), (4, 64, 0, 48), (5, 112, 0, 16)),
    ((5, 0, 16, 32), (6, 32, 0, 48), (7, 80, 0, 48)),
)


def shifted(**offsets):
    return {a: lax.rem(lax.axis_index(a) + o, SIZES[a]) for a, o in offsets.items()}


def all_peers():
    out = [{"z": dz, "c": dc} for dz in range(8) for dc in range(2) if dz or dc]
    out += [{"x": dx, "c": dc} for dx in range(1, 4) for dc in range(2)]
    out += [{"y": dy, "c": dc} for dy in range(1, 4) for dc in range(2)]
    return out


def remote(src, dst, send, recv, device):
    return pltpu.make_async_remote_copy(
        src_ref=src, dst_ref=dst, send_sem=send, recv_sem=recv, device_id=device, device_id_type=MESH
    )


def wait_bytes(ref, sem):
    pltpu.make_async_copy(ref, ref, sem).wait()


def product(low, high):
    return lax.dot_general(low, high, (((0,), (0,)), ((), ())), preferred_element_type=jnp.float32)


def kernel(
    wq, lq, hq, wk, lk, hk, wv, lv, hv, nt, ns,
    out, col_q, col_k, col_v, norm,
    weights, highs, lows, units, ready, quarters, part, got1, got2, total, norms, gathered, mean, wide, gain,
    w_sem, h_sem, l_sem, q_sem, g_sem,
    unit_sem, z_send, c_send,
    low_send, low_recv, low_send2, low_recv2, low_send3, low_recv3,
    s1_send, s1_recv, s2_send, s2_recv, s3_send, s3_recv, n3_send, n3_recv, n4_send, n4_recv,
    y_send, y_recv,
):
    z, y, c, x = (lax.axis_index(a) for a in ("z", "y", "c", "x"))
    member = 2 * y + c
    w_in, l_in, h_in = (wq, wk, wv), (lq, lk, lv), (hq, hk, hv)

    barrier = pltpu.get_barrier_semaphore()
    peers = all_peers()
    for p in peers:
        pl.semaphore_signal(barrier, inc=1, device_id=shifted(**p), device_id_type=MESH)

    loads = []
    for t in range(3):
        loads.append(
            (
                pltpu.make_async_copy(w_in[t], weights.at[t], w_sem.at[t]),
                pltpu.make_async_copy(h_in[t], highs.at[t], h_sem.at[t]),
                pltpu.make_async_copy(l_in[t], lows.at[t], l_sem.at[t]),
            )
        )
        for copy in loads[t]:
            copy.start()
    gain_loads = [pltpu.make_async_copy(ref, gain.at[n], g_sem.at[n]) for n, ref in enumerate((nt, ns))]
    for copy in gain_loads:
        copy.start()
    quarter = quarters.at[4 * c + x, 0]
    quarter_loads = []
    for t in range(3):
        copy = pltpu.make_async_copy(
            l_in[t].at[pl.ds(pl.multiple_of(16 * x, 16), 16), :],
            quarter.at[pl.ds(16 * t, 16), :],
            q_sem.at[t],
        )
        copy.start()
        quarter_loads.append(copy)

    def tile_of(turn):
        return 3 * (turn // 3) + ((y + 1) // 2 + 8 - turn) % 3

    def slot_of(k, turn):
        return 4 * k + turn // 2 if turn < 8 else 32 + k // 2

    def half(slot, core):
        return units.at[pl.ds(pl.multiple_of(384 * slot + ROWS * core, 64), ROWS), :]

    def slab(k, turn):
        first = 384 * lax.rem(z + k, 8) + TILE * (tile_of(turn) % 3)
        return weights.at[turn // 3, :, pl.ds(pl.multiple_of(first, TILE), TILE)]

    for turn in range(TILES):
        first = 384 * z + TILE * (tile_of(turn) % 3)

        @pl.when(c == turn % 2)
        def _():
            slot = slot_of(0, turn)
            src = w_in[turn // 3].at[:, pl.ds(pl.multiple_of(first, TILE), TILE)]
            pltpu.make_async_copy(src, half(slot, c), unit_sem.at[slot]).start()

    pl.semaphore_wait(barrier, len(peers))
    for copy in quarter_loads:
        copy.wait()
    for t in range(3):
        loads[t][0].wait()

    def pass_low(k, step):
        place = (k + step) % 8
        lane = 4 * c + x
        device = shifted(z=step % 8)
        remote(quarters.at[lane, k], quarters.at[lane, place], low_send, low_recv.at[place], device).start()

    def wait_low(k):
        wait_bytes(quarters.at[0, k], low_recv.at[k])

    def spread_low(*planes):
        for k in planes:
            place = quarters.at[4 * c + x, k]
            for dx in (1, 2, 3):
                remote(place, place, low_send2, low_recv2, shifted(x=dx)).start()

    pass_low(0, 1)
    pass_low(0, -1)
    for turn in range(TILES):

        @pl.when(c != turn % 2)
        def _():
            slot = slot_of(0, turn)
            remote(slab(0, turn), half(slot, c), c_send, unit_sem.at[slot], shifted(c=1)).start()

    def send_round(turn, order=Z_ORDER):
        for k in order:
            slot = slot_of(k, turn)
            device = {"z": lax.rem(z + k, 8), "c": (k + k // 4 + turn) % 2}
            remote(slab(k, turn), half(slot, c), z_send, unit_sem.at[slot], device).start()


    send_round(0, Z_ORDER[:4])
    wait_low(1)
    wait_low(7)
    pass_low(1, 1)
    pass_low(7, -1)
    send_round(0, Z_ORDER[4:])
    spread_low(0, 1, 7)

    def sum_up(t):
        low = lows[t]

        def sums(s, _):
            first = pl.ds(pl.multiple_of(384 * s, TILE), 384)
            latest = weights[t, :, first].astype(jnp.float32) + MIX_RATE * product(low[...], highs[t, :, first])
            line = jnp.sum(jnp.abs(latest), axis=0, keepdims=True)
            for j in range(3):
                part[s, pl.ds(3 * t + j, 1), :] = line[:, TILE * j : TILE * (j + 1)]
            return 0

        lax.fori_loop(0, 8, sums, 0)

    for t in range(3):
        for copy in loads[t][1:]:
            copy.wait()
    for copy in gain_loads:
        copy.wait()
    own_norm = jnp.concatenate([gain[0] + gain[1], jnp.zeros((1, 80), jnp.float32)], axis=1)
    for s in range(8):
        part[s, pl.ds(9, 1), :] = own_norm
    sum_up(0)

    sum_up(1)
    sum_up(2)

    for dy in range(4):
        for dc in range(2):
            if dy or dc:
                to = shifted(y=dy, c=dc)
                remote(part.at[2 * to["y"] + to["c"]], got1.at[member], s1_send, s1_recv, to).start()

    wait_low(2)
    wait_low(6)
    pass_low(2, 1)
    pass_low(6, -1)
    send_round(1, Z_ORDER[:4])
    spread_low(2, 6)

    got1[member] = part[member]
    wait_bytes(got1.at[pl.ds(0, 7)], s1_recv)
    mine = got1[0]
    for m in range(1, 8):
        mine = mine + got1[m]
    got2[0, pl.ds(0, 16), :] = mine
    for m in range(8):
        got2[0, pl.ds(16 + m, 1), :] = got1[m, pl.ds(9, 1), :]

    steps = lax.rem(member + 8 - z, 8)

    @pl.when(steps != 0)
    def _():
        remote(got2.at[0], got2.at[steps], s2_send, s2_recv, {"z": member}).start()

    send_round(1, Z_ORDER[4:])
    wait_low(3)
    wait_low(5)

    @pl.when(z % 2 == 1)
    def _():
        pass_low(3, 1)

    @pl.when(z % 2 == 0)
    def _():
        pass_low(5, -1)

    for turn in range(2, TILES):
        send_round(turn)
    spread_low(3, 5)
    wait_low(4)
    spread_low(4)

    wait_bytes(quarters.at[pl.ds(0, 3)], low_recv2)
    half_low = quarters.at[pl.ds(4 * c, 4)]
    remote(half_low, half_low, low_send3, low_recv3, shifted(c=1)).start()

    @pl.when(steps == 0)
    def _():
        wait_bytes(got2.at[pl.ds(0, 7)], s2_recv)
        whole = got2[0, pl.ds(0, 16), :]
        for k in range(1, 8):
            whole = whole + got2[k, pl.ds(0, 16), :]
        total[...] = whole
        for k in range(8):
            plane = lax.rem(z + 8 - k, 8)
            norms[x, pl.ds(pl.multiple_of(8 * plane, 8), 8), :] = got2[k, pl.ds(16, 8), :]
        for src, dst, send, recv in (
            (total, total, s3_send, s3_recv),
            (norms.at[x], norms.at[x], n3_send, n3_recv),
        ):
            n = 0
            for dy in range(4):
                for dc in range(2):
                    if dy or dc:
                        remote(src, dst, send.at[n], recv, shifted(y=dy, c=dc)).start()
                        n += 1

    @pl.when(steps != 0)
    def _():
        wait_bytes(total, s3_recv)
        wait_bytes(norms.at[x], n3_recv)

    for n, dx in enumerate((1, 2, 3)):
        remote(norms.at[x], norms.at[x], n4_send, n4_recv, shifted(x=dx)).start()
    mean[...] = total[...] / D_MODEL
    wait_bytes(quarters.at[pl.ds(0, 4)], low_recv3)

    own = 5 - c

    def unit(n):
        mine = n < own
        m = jnp.where(mine, 0, n - own)
        pair, place = m // 7, m % 7
        first = place < 3 + c
        index = jnp.where(first, place, place - 3 - c)
        turn = jnp.where(mine, 2 * n + c, 2 * pair + jnp.where(first, 0, 1))
        one = jnp.where(index == 0, 2, jnp.where(index == 1, 5, 7))
        other = jnp.where(index == 0, 6, jnp.where(index == 1, 3, jnp.where(index == 2, 1, 4)))
        k = jnp.where(mine, 0, jnp.where((turn + c) % 2 == 0, one, other))
        slot = jnp.where(turn == 8, 32 + k // 2, 4 * k + turn // 2)
        return k, tile_of(turn), slot

    def work(n):
        k, tile, slot = unit(n)
        tensor = tile // 3
        here = pl.ds(pl.multiple_of(384 * slot, 128), 384)
        wait_bytes(units.at[here, :], unit_sem.at[slot])
        first = 384 * z + TILE * (tile % 3)
        high = highs[tensor, :, pl.ds(pl.multiple_of(first, TILE), TILE)]
        rank = pl.ds(pl.multiple_of(16 * tensor, 16), 16)
        low = [
            jnp.concatenate([quarters[4 * core + q, k, rank, :] for q in range(4)], axis=0) for core in range(2)
        ]
        added = jnp.concatenate([product(a, high) for a in low], axis=0)
        latest = units[here, :].astype(jnp.float32) + MIX_RATE * added
        scaled = latest / mean[pl.ds(tile, 1), :]
        ready[pl.ds(pl.multiple_of(TILE * slot, TILE), TILE), :] = scaled.astype(jnp.bfloat16).T

    def hand_on(n):
        k, tile, slot = unit(n)
        tensor = tile // 3
        chip = 4 * lax.rem(z + 8 - k, 8) + y
        lanes = pl.ds(pl.multiple_of(384 * chip, 128), 384)
        for t in range(3):

            @pl.when(tile % 3 == t)
            def _():
                for owner, row, column, length in PIECES[t]:
                    src = ready.at[pl.ds(pl.multiple_of(TILE * slot + row, 16), length), :]
                    dst = out.at[tensor, pl.ds(column, length), lanes]

                    @pl.when(member == owner)
                    def _():
                        pltpu.make_async_copy(src, dst, y_recv.at[tensor]).start()

                    @pl.when(member != owner)
                    def _():
                        to = {"y": owner // 2, "c": owner % 2}
                        remote(src, dst, y_send, y_recv.at[tensor], to).start()

    def step(n, _):
        work(n)

        @pl.when(n > 0)
        def _():
            hand_on(n - 1)

        return 0

    lax.fori_loop(0, UNITS, step, 0)
    hand_on(UNITS - 1)

    for m in range(8):

        @pl.when(member == m)
        def _():
            for t in range(3):
                rows = [mean[pl.ds(3 * t + j, 1), :] for j in range(3)]
                line = jnp.concatenate(rows, axis=1)
                (col_q, col_k, col_v)[t][...] = line[:, 48 * m : 48 * m + 48]

    wait_bytes(norms.at[pl.ds(0, 3)], n4_recv)
    place = lax.broadcasted_iota(jnp.int32, (64, TILE), 1)
    n0, n1, n2, n3 = (norms[i] for i in range(4))
    r1, r2, r3 = pltpu.roll(n1, 48, 1), pltpu.roll(n2, 96, 1), pltpu.roll(n3, 16, 1)
    gathered[0] = jnp.where(place < 48, n0, jnp.where(place < 96, r1, r2))
    gathered[1] = jnp.where(place < 16, r2, r3)
    even, odd = pl.ds(0, 32, stride=2), pl.ds(1, 32, stride=2)
    a0, a1, b0, b1 = gathered[0, even, :], gathered[0, odd, :], gathered[1, even, :], gathered[1, odd, :]
    low_half = lax.broadcasted_iota(jnp.int32, (32, TILE), 1) < 64
    wide[pl.ds(0, 32, stride=3), :] = a0
    wide[pl.ds(1, 32, stride=3), :] = jnp.where(low_half, b0, pltpu.roll(a1, 64, 1))
    wide[pl.ds(2, 32, stride=3), :] = jnp.where(low_half, pltpu.roll(a1, 64, 1), pltpu.roll(b1, 64, 1))
    norm[...] = wide[...].astype(jnp.bfloat16)

    for t in range(3):
        wait_bytes(out.at[t], y_recv.at[t])
    wait_bytes(ready.at[pl.ds(0, 4032), :], y_send)
    wait_bytes(units.at[pl.ds(0, 63 * ROWS), :], z_send)

    @pl.when(c == 0)
    def _():
        wait_bytes(units.at[pl.ds(0, 4 * ROWS), :], c_send)

    @pl.when(c != 0)
    def _():
        wait_bytes(units.at[pl.ds(0, 5 * ROWS), :], c_send)

    wait_bytes(quarters.at[0, pl.ds(0, 7)], low_send)
    wait_bytes(quarters.at[pl.ds(0, 3)], low_send2)
    wait_bytes(quarters.at[pl.ds(0, 4)], low_send3)
    wait_bytes(got1.at[pl.ds(0, 7)], s1_send)
    wait_bytes(norms.at[pl.ds(0, 3)], n4_send)

    @pl.when(steps != 0)
    def _():
        wait_bytes(got2.at[0], s2_send)

    @pl.when(steps == 0)
    def _():
        for n in range(7):
            wait_bytes(total, s3_send.at[n])
            wait_bytes(norms.at[0], n3_send.at[n])


def settle(out, cq, ck, cv, norm, *results):
    *to, sem = results
    copies = [
        pltpu.make_async_copy(src, dst, sem.at[n])
        for n, (src, dst) in enumerate(zip((out.at[0], out.at[1], out.at[2], cq, ck, cv, norm), to))
    ]
    for copy in copies:
        copy.start()
    for copy in copies:
        copy.wait()


def body(wq, lq, hq, wk, lk, hk, wv, lv, hv, nt, ns):
    anywhere = pl.BlockSpec(memory_space=pltpu.HBM)
    local = pl.BlockSpec(memory_space=pltpu.VMEM)
    dma = pltpu.SemaphoreType.DMA
    bf16, f32 = jnp.bfloat16, jnp.float32
    out, *small = pl.pallas_call(
        kernel,
        name="merge_and_place",
        out_shape=(
            jax.ShapeDtypeStruct((3, 48, D_MODEL), bf16),
            *[jax.ShapeDtypeStruct((1, 48), f32)] * 3,
            jax.ShapeDtypeStruct((96, TILE), bf16),
        ),
        in_specs=[anywhere] * 11,
        out_specs=(anywhere, local, local, local, local),
        scratch_shapes=[
            pltpu.VMEM((3, ROWS, 3072), bf16),
            pltpu.VMEM((3, 64, 3072), bf16),
            pltpu.VMEM((3, 64, ROWS), bf16),
            pltpu.VMEM((UNITS * 384, TILE), bf16),
            pltpu.VMEM((UNITS * TILE, 384), bf16),
            pltpu.VMEM((8, 8, 48, ROWS), bf16),
            pltpu.VMEM((8, 16, TILE), f32),
            pltpu.VMEM((8, 16, TILE), f32),
            pltpu.VMEM((8, 24, TILE), f32),
            pltpu.VMEM((16, TILE), f32),
            pltpu.VMEM((4, 64, TILE), f32),
            pltpu.VMEM((2, 64, TILE), f32),
            pltpu.VMEM((16, TILE), f32),
            pltpu.VMEM((96, TILE), f32),
            pltpu.VMEM((2, 1, 48), f32),
            dma((3,)), dma((3,)), dma((3,)), dma((3,)), dma((2,)),
            dma((UNITS,)), dma, dma,
            dma, dma((8,)), dma, dma, dma, dma,
            dma, dma, dma, dma, dma((7,)), dma, dma((7,)), dma, dma, dma,
            dma, dma((3,)),
        ],
        compiler_params=pltpu.CompilerParams(collective_id=0, has_side_effects=True, vmem_limit_bytes=48 * 2**20),
    )(*[pltpu.with_memory_space_constraint(a, pltpu.HBM) for a in (wq, lq.T, hq, wk, lk.T, hk, wv, lv.T, hv, nt.reshape(1, -1), ns.reshape(1, -1))])
    either = pl.BlockSpec(memory_space=pl.ANY)
    q, k, v, cq, ck, cv, norm = pl.pallas_call(
        settle,
        name="settle",
        out_shape=(
            *[jax.ShapeDtypeStruct((48, D_MODEL), bf16)] * 3,
            *[jax.ShapeDtypeStruct((1, 48), f32)] * 3,
            jax.ShapeDtypeStruct((96, TILE), bf16),
        ),
        in_specs=[either] * 5,
        out_specs=[either] * 7,
        scratch_shapes=[dma((7,))],
        compiler_params=pltpu.CompilerParams(vmem_limit_bytes=2**20),
    )(out, *small)
    return q.T, k.T, v.T, cq.reshape(-1), ck.reshape(-1), cv.reshape(-1), norm.reshape(-1)


def solution(mesh):
    torus = Mesh(mesh.devices.reshape(8, 4, 2, 4), ("z", "y", "c", "x"))
    shard = ("z", "y", "c")
    in_specs = (P(shard, "x"), P(shard, None), P(None, "x")) * 3 + (P((*shard, "x")),) * 2
    columns = ("x", *shard)
    out_specs = (P(None, columns),) * 3 + (P(columns),) * 3 + (P(),)
    return jax.shard_map(body, mesh=torus, in_specs=in_specs, out_specs=out_specs, check_vma=False)
```
